512 devices in a mesh: section: 16 (over z_lo, y), seq: 32 (over x, z_hi, core).
Axes of the slice: x: 4, y: 8, z: 8 (z_hi: 4, z_lo: 2; z = z_hi * 2 + z_lo), core: 2. Of those that a mesh axis runs over, the one named last changes fastest.
Arguments:
- hidden: bfloat16 [16, 4096, 2048], P('section', 'seq'), may hold values from -6 to 6
- query_gain: bfloat16 [16, 2048], P('section'), may hold values from 0.099609375 to 1.8984375
- out_gain: bfloat16 [16, 2048], P('section'), may hold values from 0.099609375 to 1.8984375
- keys_now: bfloat16 [16, 4096, 512], P('section', 'seq'), may hold values from -26.516504 to 26.516504
- values_now: bfloat16 [16, 4096, 512], P('section', 'seq'), may hold values from -6 to 6
- keys_cached: bfloat16 [16, 4096, 512], P('section', 'seq'), may hold values from -6 to 6
- values_cached: bfloat16 [16, 4096, 512], P('section', 'seq'), may hold values from -6 to 6
- first_key: int32 [16], P('section'), may hold values from 0 to 4096
Outputs:
- handoff: bfloat16 [16, 4096, 2048], P('section', 'seq')
The draws below stay inside these ranges and needn't reach their ends.
All inputs are finite; a program needn't handle non-finite values.
Results may differ from the reference program's by a relative error of at most 0.0065.
Values may be sent and summed in bfloat16 or wider, within the bound.
No kernel may reach another device: no remote copies, remote signals or barrier semaphores. Data moves between devices by JAX's collectives and lax.ppermute only.
A program may use at most 128 MiB of HBM per device.

```python
import jax
import jax.numpy as jnp
from jax import lax

HEADS = 16
KV_HEADS = 4
HEAD = 128
SECTIONS = 16
STRETCH = 4096


def drawn(key):
    hidden_draw = jax.random.truncated_normal(jax.random.fold_in(key, 101), -6.0, 6.0, (SECTIONS, STRETCH, HEADS * HEAD), jnp.float32)
    keys_draw = jax.random.truncated_normal(jax.random.fold_in(key, 102), -6.0, 6.0, (SECTIONS, STRETCH, KV_HEADS * HEAD), jnp.float32)
    return (hidden_draw, keys_draw)


def draw_hidden(key, part):
    return drawn(key)[0].astype(jnp.bfloat16)


def draw_keys_now(key, part):
    return drawn(key)[1].astype(jnp.bfloat16)


def plant(values, key, smallest, top_value):
    place = [jax.random.randint(jax.random.fold_in(key, axis), (), 0, length) for axis, length in enumerate(values.shape)]
    widest = values.shape.index(max(values.shape))
    neighbour = place[:widest] + [(place[widest] + 1) % values.shape[widest]] + place[widest + 1:]
    return values.at[tuple(place)].set(smallest).at[tuple(neighbour)].set(top_value)


def steps_of(key, extent, cuts, least, largest):
    level = 1.0
    for position, shards_of in cuts:
        steps = jax.random.uniform(jax.random.fold_in(jax.random.fold_in(key, 6), position), (shards_of,), jnp.float32, least / len(cuts), largest / len(cuts))
        level = level * jnp.repeat(jnp.exp(steps), extent[position] // shards_of).reshape((-1,) + (1,) * (len(extent) - 1 - position))
    return level


def scatter_about(rng, extent, spread, reach, pieces=(), kind=jnp.bfloat16):
    values = spread * jax.random.normal(rng, extent, jnp.float32)
    if pieces:
        values = values * steps_of(rng, extent, pieces, -0.22, 0.18)
    return jnp.clip(values, -reach, reach).astype(kind)


def setup_inputs(seed: int = 0) -> dict:
    streams_of = jax.random.split(jax.random.key(seed), 9)
    hidden = draw_hidden(jax.random.fold_in(streams_of[8], 71), 0)
    query_gain = jnp.clip(1.0 + 0.18 * jax.random.normal(streams_of[1], (SECTIONS, HEADS * HEAD), jnp.float32), 0.099609375, 1.8984375).astype(jnp.bfloat16)
    out_gain = jnp.clip(1.0 + 0.18 * jax.random.normal(streams_of[2], (SECTIONS, HEADS * HEAD), jnp.float32), 0.099609375, 1.8984375).astype(jnp.bfloat16)
    keys_now = draw_keys_now(jax.random.fold_in(streams_of[8], 71), 0)
    values_now = scatter_about(streams_of[4], (SECTIONS, STRETCH, KV_HEADS * HEAD), 1.0, 6.0, ((0, 16), (1, 32)))
    keys_cached = scatter_about(streams_of[5], (SECTIONS, STRETCH, KV_HEADS * HEAD), 1.0, 6.0, ((0, 16), (1, 32)))
    values_cached = scatter_about(streams_of[6], (SECTIONS, STRETCH, KV_HEADS * HEAD), 1.0, 6.0, ((0, 16), (1, 32)))
    first_key = plant(jax.random.randint(streams_of[7], (SECTIONS,), 0, STRETCH + 1), jax.random.fold_in(streams_of[7], 1), 0, STRETCH).astype(jnp.int32)
    return dict(hidden=hidden, query_gain=query_gain, out_gain=out_gain, keys_now=keys_now, values_now=values_now, keys_cached=keys_cached, values_cached=values_cached, first_key=first_key)


masked_score = -1e+30

def rms_scale(values):
    return lax.rsqrt(lax.optimization_barrier(jnp.mean(values * values, axis=-1, keepdims=True)) + 1e-06)

def one_section(inputs):
    hidden, query_gain, out_gain, keys_now, values_now, keys_cached, values_cached, first_key = inputs
    widened = hidden.astype(jnp.float32)
    queries = (widened * rms_scale(widened) * query_gain.astype(jnp.float32)).astype(jnp.bfloat16)
    grouped = queries.reshape(STRETCH, KV_HEADS, HEADS // KV_HEADS, HEAD)
    all_keys = jnp.concatenate([keys_cached, keys_now], 0).reshape(2 * STRETCH, KV_HEADS, HEAD)
    all_values = jnp.concatenate([values_cached, values_now], 0).reshape(2 * STRETCH, KV_HEADS, HEAD)
    block_rows = min(512, STRETCH)
    score_scale = HEAD ** (-0.5)

    def attend(block_start):
        query_block = lax.dynamic_slice_in_dim(grouped, block_start, block_rows, 0)
        key_block = lax.dynamic_slice_in_dim(all_keys, block_start, STRETCH + block_rows, 0)
        value_block = lax.dynamic_slice_in_dim(all_values, block_start, STRETCH + block_rows, 0)
        scores = jnp.einsum('tgqd,bgd->gqtb', query_block.astype(jnp.float32), key_block.astype(jnp.float32)) * score_scale
        positions = block_start + jnp.arange(block_rows, dtype=jnp.int32)
        columns = block_start + jnp.arange(STRETCH + block_rows, dtype=jnp.int32)
        visible = (columns[None, :] > positions[:, None]) & (columns[None, :] <= positions[:, None] + STRETCH) & (columns[None, :] >= first_key)
        scores = jnp.where(visible, scores, masked_score)
        highest = lax.optimization_barrier(jnp.max(scores, axis=-1, keepdims=True))
        weights = jnp.exp(scores - highest)
        totals = lax.optimization_barrier(jnp.sum(weights, axis=-1))
        rounded = lax.optimization_barrier(weights.astype(jnp.bfloat16)).astype(jnp.float32)
        summed = jnp.einsum('gqtb,bgd->gqtd', rounded, value_block.astype(jnp.float32))
        attended = (summed / totals[..., None]).astype(jnp.bfloat16)
        return jnp.transpose(attended, (2, 0, 1, 3)).reshape(block_rows, HEADS * HEAD)
    starts = (jnp.arange(STRETCH // block_rows) * block_rows).astype(jnp.int32)
    attended = lax.map(attend, starts).reshape(STRETCH, HEADS * HEAD).astype(jnp.float32)
    branch = attended * rms_scale(attended) * out_gain.astype(jnp.float32)
    return (widened + branch).astype(jnp.bfloat16)

def reference(hidden, query_gain, out_gain, keys_now, values_now, keys_cached, values_cached, first_key):
    layered = lax.map(one_section, (hidden, query_gain, out_gain, keys_now, values_now, keys_cached, values_cached, first_key))
    return jnp.roll(layered, 1, axis=0)
```

```python
import functools
import math

import jax
import jax.numpy as jnp
from jax import lax
from jax.experimental import pallas as pl
from jax.experimental.pallas import tpu as pltpu
from jax.sharding import PartitionSpec as P

HEADS = 16
KV_HEADS = 4
HEAD = 128
GROUP = HEADS // KV_HEADS
BLK = 128
XS = 4
ZS = 4
SECTIONS = 16
SEQ = 32
MASKED = -1e30
EXP2_SCALE = HEAD**-0.5 * math.log2(math.e)
ROUNDS = (0, 1, 3, 2)
TILE = 256
BLOCKS = 33


def seq_of(x, z, c):
    return (x % XS) * 8 + (z % ZS) * 2 + c


def sign(c):
    return 1 - 2 * c


def along_z(r):
    return [(seq_of(x, z, c), seq_of(x, z + sign(c) * r, c)) for x in range(XS) for z in range(ZS) for c in range(2)]


def along_x(r):
    return [(seq_of(x, z, c), seq_of(x + sign(c) * r, z, c)) for x in range(XS) for z in range(ZS) for c in range(2)]


def home_pairs(r):
    return [
        (s * SEQ + seq_of(x, z, c), (s + 1) % SECTIONS * SEQ + seq_of(x, z - sign(c) * r, c))
        for s in range(SECTIONS)
        for x in range(XS)
        for z in range(ZS)
        for c in range(2)
    ]


OTHER_CORE = [(q, q ^ 1) for q in range(SEQ)]


def nt(a, b):
    return lax.dot_general(a, b, (((1,), (1,)), ((), ())), preferred_element_type=jnp.float32)


def attention_kernel(meta, q_ref, own_ref, other_ref, far_ref, far_other_ref, o_ref, s_ref, *, kq):
    cols = lax.broadcasted_iota(jnp.int32, (BLK, BLK), 1)
    rows = lax.broadcasted_iota(jnp.int32, (BLK, BLK), 0)
    limit, me = meta[0], meta[1]
    x, z, c = me // 8, (me // 2) % 4, me % 2
    sg = 1 - 2 * c
    row_base = x * 8 * BLK
    place = [[2 * ((z - flip * r + 4) % 4) + core for r in ROUNDS] for flip, core in ((sg, c), (-sg, 1 - c))]
    diag = place[0][kq]
    heads = TILE // BLK
    blocks = []
    for half, ref in ((0, far_ref), (1, far_other_ref)):
        flip = -sg if half else sg
        for i in range(3):
            source = (x - flip * ROUNDS[i + 1] + 4) % 4
            for k in range(4):
                start = jnp.where(source > x, limit - BLK * (8 * source + place[half][k]), 0)
                blocks.append((ref, (i, k, 0), (i, k, 1), cols >= start))
    for half, ref in ((0, own_ref), (1, other_ref)):
        for k in range(4):
            if half == 0 and k == kq:
                continue
            at = place[half][k]
            cached = (at > diag).astype(jnp.int32) * 2
            start = jnp.where(at > diag, limit - (row_base + at * BLK), 0)
            blocks.append((ref, (k, cached), (k, cached + 1), cols >= start))
    blocks.append((own_ref, (kq, 0), (kq, 1), cols <= rows))
    blocks.append((own_ref, (kq, 2), (kq, 3), (cols > rows) & (cols >= limit - (row_base + diag * BLK))))
    pairs = [blocks[j : j + 2] for j in range(0, len(blocks), 2)]
    for t in range(GROUP // heads):
        q = jnp.concatenate([q_ref[:, (t * heads + h) * BLK : (t * heads + h + 1) * BLK] for h in range(heads)], 0)
        best = None
        for j, pair in enumerate(pairs):
            scores = nt(q, jnp.concatenate([ref[k_at] for ref, k_at, _, _ in pair], 0))
            for u, (_, _, _, mask) in enumerate(pair):
                part = jnp.where(jnp.concatenate([mask] * heads, 0), scores[:, u * BLK : (u + 1) * BLK], MASKED)
                s_ref[t % 2, :, (2 * j + u) * BLK : (2 * j + u + 1) * BLK] = part
                best = part if best is None else jnp.maximum(best, part)
        highest = jnp.max(best, axis=1, keepdims=True) * EXP2_SCALE
        total = None
        for j, pair in enumerate(pairs):
            span = s_ref[t % 2, :, 2 * j * BLK : (2 * j + len(pair)) * BLK]
            weights = jnp.exp2(span * EXP2_SCALE - highest)
            values = jnp.concatenate([ref[v_at] for ref, _, v_at, _ in pair], 0)
            values = jnp.concatenate([values, jnp.ones_like(values)], 1)
            part = jnp.dot(weights.astype(jnp.bfloat16), values, preferred_element_type=jnp.float32)
            total = part if total is None else total + part
        out = (total[:, :BLK] / total[:, BLK:]).astype(jnp.bfloat16)
        for h in range(heads):
            o_ref[:, (t * heads + h) * BLK : (t * heads + h + 1) * BLK] = out[h * BLK : (h + 1) * BLK]


def attend(meta, q, own, other, far, far_other, kq):
    vmem = pl.BlockSpec(memory_space=pltpu.VMEM)
    return pl.pallas_call(
        functools.partial(attention_kernel, kq=kq),
        out_shape=jax.ShapeDtypeStruct((BLK, GROUP * HEAD), jnp.bfloat16),
        in_specs=[pl.BlockSpec(memory_space=pltpu.SMEM)] + [vmem] * 5,
        out_specs=vmem,
        scratch_shapes=[pltpu.VMEM((2, TILE, BLOCKS * BLK), jnp.float32)],
        compiler_params=pltpu.CompilerParams(vmem_limit_bytes=24 * 2**20),
        cost_estimate=pl.CostEstimate(flops=4 * 512 * 4096 * 128, bytes_accessed=2**20, transcendentals=0),
        name="attend",
    )(meta, q, own, other, far, far_other)


def finish_kernel(meta, o0, o1, o2, o3, hidden_ref, out_ref):
    parts = [o[...].astype(jnp.float32) for o in (o0, o1, o2, o3)]
    squares = None
    for part in parts:
        part = part * part
        part = part[:, :128] + part[:, 128:256] + part[:, 256:384] + part[:, 384:]
        squares = part if squares is None else squares + part
    scale = lax.rsqrt(jnp.sum(squares, axis=1, keepdims=True) / (HEADS * HEAD) + 1e-06)
    z, c = (meta[1] // 2) % 4, meta[1] % 2
    for r, part in zip(ROUNDS, parts):
        at = pl.ds(pl.multiple_of((z + (1 - 2 * c) * r + 4) % 4 * 512, 512), 512)
        gain = hidden_ref[BLK : BLK + 16, at].astype(jnp.float32)[:1]
        out_ref[0, :, at] = (hidden_ref[:BLK, at].astype(jnp.float32) + part * scale * gain).astype(jnp.bfloat16)


def finish(meta, parts, hidden_and_gain):
    vmem = pl.BlockSpec(memory_space=pltpu.VMEM)
    return pl.pallas_call(
        finish_kernel,
        out_shape=jax.ShapeDtypeStruct((1, BLK, HEADS * HEAD), jnp.bfloat16),
        in_specs=[pl.BlockSpec(memory_space=pltpu.SMEM)] + [vmem] * 5,
        out_specs=vmem,
        compiler_params=pltpu.CompilerParams(vmem_limit_bytes=16 * 2**20),
        name="finish",
    )(meta, *parts, hidden_and_gain)


def on_device(hidden, query_gain, out_gain, keys_now, values_now, keys_cached, values_cached, first_key):
    me = lax.axis_index("seq")
    x, z, c = me // 8, (me // 2) % 4, me % 2
    sg = 1 - 2 * c
    limit = first_key[0]

    def kv_of(head):
        return jnp.stack(
            [
                lax.dynamic_slice(a[0], (0, head * HEAD), (BLK, HEAD))
                for a in (keys_now, values_now, keys_cached, values_cached)
            ]
        )

    own = jnp.stack(
        [kv_of(z)] + [lax.ppermute(kv_of((z + sg * r) % 4), "seq", along_z(r)) for r in ROUNDS[1:]]
    )
    other = lax.ppermute(own, "seq", OTHER_CORE)
    far = []
    for r in ROUNDS[1:]:
        target = (x + sg * r) % 4
        picked = lax.dynamic_slice_in_dim(own, jnp.where(target > x, 0, 2), 2, 1)
        far.append(lax.ppermute(picked, "seq", along_x(r)))
    far = jnp.stack(far)
    far_other = lax.ppermute(far, "seq", OTHER_CORE)

    widened = hidden[0].astype(jnp.float32)
    scale = lax.rsqrt(jnp.mean(widened * widened, axis=-1, keepdims=True) + 1e-06)
    queries = (widened * scale * query_gain[0].astype(jnp.float32)).astype(jnp.bfloat16)

    def q_of(head):
        return lax.dynamic_slice(queries, (0, head * GROUP * HEAD), (BLK, GROUP * HEAD))

    qs = [q_of(z)] + [lax.ppermute(q_of((z + sg * r) % 4), "seq", along_z(r)) for r in ROUNDS[1:]]

    gain_rows = jnp.broadcast_to(out_gain, (16, HEADS * HEAD))
    before = [(s, (s + 1) % SECTIONS) for s in range(SECTIONS)]
    hidden_before = lax.ppermute(jnp.concatenate([hidden[0], gain_rows], 0), "section", before)

    meta = jnp.stack([limit, me])

    parts = []
    for k, r in enumerate(ROUNDS):
        attended = attend(meta, qs[k], own, other, far, far_other, k)
        parts.append(lax.ppermute(attended, ("section", "seq"), home_pairs(r)))
    return finish(meta, parts, hidden_before)


def solution(mesh):
    assert mesh.shape["section"] == SECTIONS and mesh.shape["seq"] == SEQ
    return jax.shard_map(
        on_device,
        mesh=mesh,
        in_specs=(
            P("section", "seq", None),
            P("section", None),
            P("section", None),
            P("section", "seq", None),
            P("section", "seq", None),
            P("section", "seq", None),
            P("section", "seq", None),
            P("section"),
        ),
        out_specs=P("section", "seq", None),
        check_vma=False,
    )
```

```python
import functools
import math

import jax
import jax.numpy as jnp
from jax import lax
from jax.experimental import pallas as pl
from jax.experimental.pallas import tpu as pltpu
from jax.sharding import PartitionSpec as P


HEADS = 16
KV_HEADS = 4
HEAD = 128
GROUP = HEADS // KV_HEADS
BLK = 128
XS = 4
ZS = 4
SECTIONS = 16
SEQ = 32
MASKED = -1e30
EXP2_SCALE = HEAD**-0.5 * math.log2(math.e)
ROUNDS = (0, 1, 3, 2)
TILE = 256
BLOCKS = 33


def seq_of(x, z, c):
    return (x % XS) * 8 + (z % ZS) * 2 + c


def sign(c):
    return 1 - 2 * c


def along_z(r):
    return [(seq_of(x, z, c), seq_of(x, z + sign(c) * r, c)) for x in range(XS) for z in range(ZS) for c in range(2)]


def along_x(r):
    return [(seq_of(x, z, c), seq_of(x + sign(c) * r, z, c)) for x in range(XS) for z in range(ZS) for c in range(2)]


def home_pairs(r):
    return [
        (s * SEQ + seq_of(x, z, c), (s + 1) % SECTIONS * SEQ + seq_of(x, z - sign(c) * r, c))
        for s in range(SECTIONS)
        for x in range(XS)
        for z in range(ZS)
        for c in range(2)
    ]


OTHER_CORE = [(q, q ^ 1) for q in range(SEQ)]


def nt(a, b):
    return lax.dot_general(a, b, (((1,), (1,)), ((), ())), preferred_element_type=jnp.float32)


def attention_kernel(meta, q_ref, own_ref, other_ref, far_ref, far_other_ref, o_ref, s_ref, *, kq):
    cols = lax.broadcasted_iota(jnp.int32, (BLK, BLK), 1)
    rows = lax.broadcasted_iota(jnp.int32, (BLK, BLK), 0)
    limit, me = meta[0], meta[1]
    x, z, c = me // 8, (me // 2) % 4, me % 2
    sg = 1 - 2 * c
    row_base = x * 8 * BLK
    place = [[2 * ((z - flip * r + 4) % 4) + core for r in ROUNDS] for flip, core in ((sg, c), (-sg, 1 - c))]
    diag = place[0][kq]
    heads = TILE // BLK
    blocks = []
    for half, ref in ((0, far_ref), (1, far_other_ref)):
        flip = -sg if half else sg
        for i in range(3):
            source = (x - flip * ROUNDS[i + 1] + 4) % 4
            for k in range(4):
                start = jnp.where(source > x, limit - BLK * (8 * source + place[half][k]), 0)
                blocks.append((ref, (i, k, 0), (i, k, 1), cols >= start))
    for half, ref in ((0, own_ref), (1, other_ref)):
        for k in range(4):
            if half == 0 and k == kq:
                continue
            at = place[half][k]
            cached = (at > diag).astype(jnp.int32) * 2
            start = jnp.where(at > diag, limit - (row_base + at * BLK), 0)
            blocks.append((ref, (k, cached), (k, cached + 1), cols >= start))
    blocks.append((own_ref, (kq, 0), (kq, 1), cols <= rows))
    blocks.append((own_ref, (kq, 2), (kq, 3), (cols > rows) & (cols >= limit - (row_base + diag * BLK))))
    pairs = [blocks[j : j + 2] for j in range(0, len(blocks), 2)]
    for t in range(GROUP // heads):
        q = jnp.concatenate([q_ref[:, (t * heads + h) * BLK : (t * heads + h + 1) * BLK] for h in range(heads)], 0)
        best = None
        for j, pair in enumerate(pairs):
            scores = nt(q, jnp.concatenate([ref[k_at] for ref, k_at, _, _ in pair], 0))
            for u, (_, _, _, mask) in enumerate(pair):
                part = jnp.where(jnp.concatenate([mask] * heads, 0), scores[:, u * BLK : (u + 1) * BLK], MASKED)
                s_ref[t % 2, :, (2 * j + u) * BLK : (2 * j + u + 1) * BLK] = part
                best = part if best is None else jnp.maximum(best, part)
        highest = jnp.max(best, axis=1, keepdims=True) * EXP2_SCALE
        total = None
        for j, pair in enumerate(pairs):
            span = s_ref[t % 2, :, 2 * j * BLK : (2 * j + len(pair)) * BLK]
            weights = jnp.exp2(span * EXP2_SCALE - highest)
            values = jnp.concatenate([ref[v_at] for ref, _, v_at, _ in pair], 0)
            values = jnp.concatenate([values, jnp.ones_like(values)], 1)
            part = jnp.dot(weights.astype(jnp.bfloat16), values, preferred_element_type=jnp.float32)
            total = part if total is None else total + part
        out = (total[:, :BLK] / total[:, BLK:]).astype(jnp.bfloat16)
        for h in range(heads):
            o_ref[:, (t * heads + h) * BLK : (t * heads + h + 1) * BLK] = out[h * BLK : (h + 1) * BLK]


def attend(meta, q, own, other, far, far_other, kq):
    vmem = pl.BlockSpec(memory_space=pltpu.VMEM)
    return pl.pallas_call(
        functools.partial(attention_kernel, kq=kq),
        out_shape=jax.ShapeDtypeStruct((BLK, GROUP * HEAD), jnp.bfloat16),
        in_specs=[pl.BlockSpec(memory_space=pltpu.SMEM)] + [vmem] * 5,
        out_specs=vmem,
        scratch_shapes=[pltpu.VMEM((2, TILE, BLOCKS * BLK), jnp.float32)],
        compiler_params=pltpu.CompilerParams(vmem_limit_bytes=24 * 2**20),
        cost_estimate=pl.CostEstimate(flops=4 * 512 * 4096 * 128, bytes_accessed=2**20, transcendentals=0),
        name="attend",
    )(meta, q, own, other, far, far_other)


def finish_kernel(meta, o0, o1, o2, o3, hidden_ref, out_ref):
    parts = [o[...].astype(jnp.float32) for o in (o0, o1, o2, o3)]
    squares = None
    for part in parts:
        part = part * part
        part = part[:, :128] + part[:, 128:256] + part[:, 256:384] + part[:, 384:]
        squares = part if squares is None else squares + part
    scale = lax.rsqrt(jnp.sum(squares, axis=1, keepdims=True) / (HEADS * HEAD) + 1e-06)
    z, c = (meta[1] // 2) % 4, meta[1] % 2
    for r, part in zip(ROUNDS, parts):
        at = pl.ds(pl.multiple_of((z + (1 - 2 * c) * r + 4) % 4 * 512, 512), 512)
        gain = hidden_ref[BLK : BLK + 16, at].astype(jnp.float32)[:1]
        out_ref[0, :, at] = (hidden_ref[:BLK, at].astype(jnp.float32) + part * scale * gain).astype(jnp.bfloat16)


def finish(meta, parts, hidden_and_gain):
    vmem = pl.BlockSpec(memory_space=pltpu.VMEM)
    return pl.pallas_call(
        finish_kernel,
        out_shape=jax.ShapeDtypeStruct((1, BLK, HEADS * HEAD), jnp.bfloat16),
        in_specs=[pl.BlockSpec(memory_space=pltpu.SMEM)] + [vmem] * 5,
        out_specs=vmem,
        compiler_params=pltpu.CompilerParams(vmem_limit_bytes=16 * 2**20),
        name="finish",
    )(meta, *parts, hidden_and_gain)


def on_device(hidden, query_gain, out_gain, keys_now, values_now, keys_cached, values_cached, first_key):
    me = lax.axis_index("seq")
    x, z, c = me // 8, (me // 2) % 4, me % 2
    sg = 1 - 2 * c
    limit = first_key[0]

    def kv_of(head):
        return jnp.stack(
            [
                lax.dynamic_slice(a[0], (0, head * HEAD), (BLK, HEAD))
                for a in (keys_now, values_now, keys_cached, values_cached)
            ]
        )

    pieces = [kv_of(z)]
    for k, r in enumerate(ROUNDS[1:], 1):
        pieces.append(lax.ppermute(kv_of((z + sg * r) % 4), "seq", along_z(r)))
    own = jnp.stack(pieces)

    widened = hidden[0].astype(jnp.float32)
    scale = lax.rsqrt(jnp.mean(widened * widened, axis=-1, keepdims=True) + 1e-06)
    queries = (widened * scale * query_gain[0].astype(jnp.float32)).astype(jnp.bfloat16)

    def q_of(head):
        return lax.dynamic_slice(queries, (0, head * GROUP * HEAD), (BLK, GROUP * HEAD))

    qs = [q_of(z)]
    for k, r in enumerate(ROUNDS[1:], 1):
        qs.append(lax.ppermute(q_of((z + sg * r) % 4), "seq", along_z(r)))

    far = []
    for k, r in enumerate(ROUNDS[1:], 1):
        target = (x + sg * r) % 4
        picked = lax.dynamic_slice_in_dim(own, jnp.where(target > x, 0, 2), 2, 1)
        far.append(lax.ppermute(picked, "seq", along_x(r)))
    other = lax.ppermute(own, "seq", OTHER_CORE)
    far = jnp.stack(far)
    far_other = lax.ppermute(far, "seq", OTHER_CORE)

    gain_rows = jnp.broadcast_to(out_gain, (16, HEADS * HEAD))
    before = [(s, (s + 1) % SECTIONS) for s in range(SECTIONS)]
    hidden_before = lax.ppermute(jnp.concatenate([hidden[0], gain_rows], 0), "section", before)

    meta = jnp.stack([limit, me])
    parts = [None] * 4
    for k in (0, 1, 3, 2):
        attended = attend(meta, qs[k], own, other, far, far_other, k)
        parts[k] = lax.ppermute(attended, ("section", "seq"), home_pairs(ROUNDS[k]))
    return finish(meta, parts, hidden_before)


def solution(mesh):
    assert mesh.shape["section"] == SECTIONS and mesh.shape["seq"] == SEQ

    return jax.shard_map(
        on_device,
        mesh=mesh,
        in_specs=(
            P("section", "seq", None),
            P("section", None),
            P("section", None),
            P("section", "seq", None),
            P("section", "seq", None),
            P("section", "seq", None),
            P("section", "seq", None),
            P("section"),
        ),
        out_specs=P("section", "seq", None),
        check_vma=False,
    )
```

```python
import functools
import math

import jax
import jax.numpy as jnp
from jax import lax
from jax.experimental import pallas as pl
from jax.experimental.pallas import tpu as pltpu
from jax.sharding import PartitionSpec as P


HEADS = 16
KV_HEADS = 4
HEAD = 128
GROUP = HEADS // KV_HEADS
BLK = 128
XS = 4
ZS = 4
SECTIONS = 16
SEQ = 32
MASKED = -1e30
EXP2_SCALE = HEAD**-0.5 * math.log2(math.e)
ROUNDS = (0, 1, 3, 2)
TILE = 256
BLOCKS = 33
GAIN_ROWS = 16 * KV_HEADS


def seq_of(x, z, c):
    return (x % XS) * 8 + (z % ZS) * 2 + c


def sign(c):
    return 1 - 2 * c


def along_z(r):
    return [(seq_of(x, z, c), seq_of(x, z + sign(c) * r, c)) for x in range(XS) for z in range(ZS) for c in range(2)]


def along_x(r):
    return [(seq_of(x, z, c), seq_of(x + sign(c) * r, z, c)) for x in range(XS) for z in range(ZS) for c in range(2)]


def home_pairs(r):
    return [
        (s * SEQ + seq_of(x, z, c), (s + 1) % SECTIONS * SEQ + seq_of(x, z - sign(c) * r, c))
        for s in range(SECTIONS)
        for x in range(XS)
        for z in range(ZS)
        for c in range(2)
    ]


Z_GROUPS = [[seq_of(x, z, c) for z in range(ZS)] for x in range(XS) for c in range(2)]
OTHER_CORE = [(q, q ^ 1) for q in range(SEQ)]


def nt(a, b):
    return lax.dot_general(a, b, (((1,), (1,)), ((), ())), preferred_element_type=jnp.float32)


def attention_kernel(meta, q_ref, own_ref, other_ref, far_ref, far_other_ref, gain_ref, o_ref, s_ref, *, kq):
    cols = lax.broadcasted_iota(jnp.int32, (BLK, BLK), 1)
    rows = lax.broadcasted_iota(jnp.int32, (BLK, BLK), 0)
    limit, me = meta[0], meta[1]
    x, z, c = me // 8, (me // 2) % 4, me % 2
    sg = 1 - 2 * c
    row_base = x * 8 * BLK
    place = [[2 * ((z - flip * r + 4) % 4) + core for r in ROUNDS] for flip, core in ((sg, c), (-sg, 1 - c))]
    diag = place[0][kq]
    heads = TILE // BLK
    q_at = z if kq == 0 else (z - sg * ROUNDS[kq] + 4) % 4
    blocks = []
    for half, ref in ((0, far_ref), (1, far_other_ref)):
        flip = -sg if half else sg
        for i in range(3):
            source = (x - flip * ROUNDS[i + 1] + 4) % 4
            for k in range(4):
                start = jnp.where(source > x, limit - BLK * (8 * source + place[half][k]), 0)
                blocks.append((ref, (i, k, 0), (i, k, 1), cols >= start))
    for half, ref in ((0, own_ref), (1, other_ref)):
        for k in range(4):
            if half == 0 and k == kq:
                continue
            at = place[half][k]
            cached = (at > diag).astype(jnp.int32) * 2
            start = jnp.where(at > diag, limit - (row_base + at * BLK), 0)
            blocks.append((ref, (k, cached), (k, cached + 1), cols >= start))
    blocks.append((own_ref, (kq, 0), (kq, 1), cols <= rows))
    blocks.append((own_ref, (kq, 2), (kq, 3), (cols > rows) & (cols >= limit - (row_base + diag * BLK))))
    pairs = [blocks[j : j + 2] for j in range(0, len(blocks), 2)]
    for t in range(GROUP // heads):
        lanes = [slice((t * heads + h) * BLK, (t * heads + h + 1) * BLK) for h in range(heads)]
        q = jnp.concatenate([q_ref[q_at, :, lane] for lane in lanes], 0)
        best = None
        for j, pair in enumerate(pairs):
            scores = nt(q, jnp.concatenate([ref[k_at] for ref, k_at, _, _ in pair], 0))
            for u, (_, _, _, mask) in enumerate(pair):
                part = jnp.where(jnp.concatenate([mask] * heads, 0), scores[:, u * BLK : (u + 1) * BLK], MASKED)
                s_ref[t % 2, :, (2 * j + u) * BLK : (2 * j + u + 1) * BLK] = part
                best = part if best is None else jnp.maximum(best, part)
        highest = jnp.max(best, axis=1, keepdims=True) * EXP2_SCALE
        total = None
        for j, pair in enumerate(pairs):
            span = s_ref[t % 2, :, 2 * j * BLK : (2 * j + len(pair)) * BLK]
            weights = jnp.exp2(span * EXP2_SCALE - highest)
            values = jnp.concatenate([ref[v_at] for ref, _, v_at, _ in pair], 0)
            values = jnp.concatenate([values, jnp.ones_like(values)], 1)
            part = jnp.dot(weights.astype(jnp.bfloat16), values, preferred_element_type=jnp.float32)
            total = part if total is None else total + part
        out = (total[:, :BLK] / total[:, BLK:]).astype(jnp.bfloat16)
        for h in range(heads):
            o_ref[:BLK, (t * heads + h) * BLK : (t * heads + h + 1) * BLK] = out[h * BLK : (h + 1) * BLK]
    if kq == 0:
        for g in range(KV_HEADS):
            rows_of = slice(BLK + 16 * g, BLK + 16 * (g + 1))
            part = gain_ref[:, g * GROUP * HEAD : (g + 1) * GROUP * HEAD].astype(jnp.float32)
            o_ref[rows_of, :] = jnp.broadcast_to(part, (16, GROUP * HEAD)).astype(jnp.bfloat16)


def attend(meta, q, own, other, far, far_other, kq, gain):
    vmem = pl.BlockSpec(memory_space=pltpu.VMEM)
    rows = BLK + GAIN_ROWS if kq == 0 else BLK
    return pl.pallas_call(
        functools.partial(attention_kernel, kq=kq),
        out_shape=jax.ShapeDtypeStruct((rows, GROUP * HEAD), jnp.bfloat16),
        in_specs=[pl.BlockSpec(memory_space=pltpu.SMEM)] + [vmem] * 6,
        out_specs=vmem,
        scratch_shapes=[pltpu.VMEM((2, TILE, BLOCKS * BLK), jnp.float32)],
        compiler_params=pltpu.CompilerParams(vmem_limit_bytes=24 * 2**20),
        cost_estimate=pl.CostEstimate(flops=4 * 512 * 4096 * 128, bytes_accessed=2**20, transcendentals=0),
        name="attend",
    )(meta, q, own, other, far, far_other, gain)


def finish_kernel(meta, o0, o1, o2, o3, hidden_ref, out_ref):
    parts = [o[:BLK].astype(jnp.float32) for o in (o0, o1, o2, o3)]
    squares = None
    for part in parts:
        part = part * part
        part = part[:, :128] + part[:, 128:256] + part[:, 256:384] + part[:, 384:]
        squares = part if squares is None else squares + part
    scale = lax.rsqrt(jnp.sum(squares, axis=1, keepdims=True) / (HEADS * HEAD) + 1e-06)
    z, c = (meta[1] // 2) % 4, meta[1] % 2
    for r, part in zip(ROUNDS, parts):
        group = (z + (1 - 2 * c) * r + 4) % 4
        at = pl.ds(pl.multiple_of(group * 512, 512), 512)
        gain = o0[pl.ds(pl.multiple_of(BLK + 16 * group, 16), 16), :].astype(jnp.float32)[:1]
        out_ref[0, :, at] = (hidden_ref[0, :, at].astype(jnp.float32) + part * scale * gain).astype(jnp.bfloat16)


def finish(meta, parts, hidden_before):
    vmem = pl.BlockSpec(memory_space=pltpu.VMEM)
    return pl.pallas_call(
        finish_kernel,
        out_shape=jax.ShapeDtypeStruct((1, BLK, HEADS * HEAD), jnp.bfloat16),
        in_specs=[pl.BlockSpec(memory_space=pltpu.SMEM)] + [vmem] * 5,
        out_specs=vmem,
        compiler_params=pltpu.CompilerParams(vmem_limit_bytes=16 * 2**20),
        name="finish",
    )(meta, *parts, hidden_before)


def on_device(hidden, query_gain, out_gain, keys_now, values_now, keys_cached, values_cached, first_key):
    me = lax.axis_index("seq")
    x, z, c = me // 8, (me // 2) % 4, me % 2
    sg = 1 - 2 * c
    limit = first_key[0]

    def kv_of(head):
        return jnp.stack(
            [
                lax.dynamic_slice(a[0], (0, head * HEAD), (BLK, HEAD))
                for a in (keys_now, values_now, keys_cached, values_cached)
            ]
        )

    hidden_before = lax.ppermute(hidden, "section", [(s, (s + 1) % SECTIONS) for s in range(SECTIONS)])
    pieces = [kv_of(z)]
    for k, r in enumerate(ROUNDS[1:], 1):
        pieces.append(lax.ppermute(kv_of((z + sg * r) % 4), "seq", along_z(r)))
    own = jnp.stack(pieces)

    widened = hidden[0].astype(jnp.float32)
    scale = lax.rsqrt(jnp.mean(widened * widened, axis=-1, keepdims=True) + 1e-06)
    queries = (widened * scale * query_gain[0].astype(jnp.float32)).astype(jnp.bfloat16)
    by_group = jnp.transpose(queries.reshape(BLK, KV_HEADS, GROUP * HEAD), (1, 0, 2))
    gathered = lax.all_to_all(by_group, "seq", 0, 0, axis_index_groups=Z_GROUPS)

    far = []
    for k, r in enumerate(ROUNDS[1:], 1):
        target = (x + sg * r) % 4
        picked = lax.dynamic_slice_in_dim(own, jnp.where(target > x, 0, 2), 2, 1)
        far.append(lax.ppermute(picked, "seq", along_x(r)))
    other = lax.ppermute(own, "seq", OTHER_CORE)
    far = jnp.stack(far)
    far_other = lax.ppermute(far, "seq", OTHER_CORE)

    meta = jnp.stack([limit, me])
    parts = [None] * 4
    for k in (0, 3, 1, 2):
        attended = attend(meta, gathered if k else by_group, own, other, far, far_other, k, out_gain)
        parts[k] = lax.ppermute(attended, ("section", "seq"), home_pairs(ROUNDS[k]))
    return finish(meta, parts, hidden_before)


def solution(mesh):
    assert mesh.shape["section"] == SECTIONS and mesh.shape["seq"] == SEQ

    return jax.shard_map(
        on_device,
        mesh=mesh,
        in_specs=(
            P("section", "seq", None),
            P("section", None),
            P("section", None),
            P("section", "seq", None),
            P("section", "seq", None),
            P("section", "seq", None),
            P("section", "seq", None),
            P("section"),
        ),
        out_specs=P("section", "seq", None),
        check_vma=False,
    )
```

```python
import functools
import math

import jax
import jax.numpy as jnp
from jax import lax
from jax.experimental import pallas as pl
from jax.experimental.pallas import tpu as pltpu
from jax.sharding import PartitionSpec as P


HEADS = 16
KV_HEADS = 4
HEAD = 128
GROUP = HEADS // KV_HEADS
BLK = 128
XS = 4
ZS = 4
SECTIONS = 16
SEQ = 32
MASKED = -1e30
EXP2_SCALE = HEAD**-0.5 * math.log2(math.e)
ROUNDS = (0, 1, 3, 2)
TILE = 256
BLOCKS = 33
GAIN_ROWS = 16 * KV_HEADS


def seq_of(x, z, c):
    return (x % XS) * 8 + (z % ZS) * 2 + c


def sign(c):
    return 1 - 2 * c


def along_z(r):
    return [(seq_of(x, z, c), seq_of(x, z + sign(c) * r, c)) for x in range(XS) for z in range(ZS) for c in range(2)]


def along_x(r):
    return [(seq_of(x, z, c), seq_of(x + sign(c) * r, z, c)) for x in range(XS) for z in range(ZS) for c in range(2)]


def home_pairs(r):
    return [
        (s * SEQ + seq_of(x, z, c), (s + 1) % SECTIONS * SEQ + seq_of(x, z - sign(c) * r, c))
        for s in range(SECTIONS)
        for x in range(XS)
        for z in range(ZS)
        for c in range(2)
    ]


OTHER_CORE = [(q, q ^ 1) for q in range(SEQ)]


def nt(a, b):
    return lax.dot_general(a, b, (((1,), (1,)), ((), ())), preferred_element_type=jnp.float32)


def attention_kernel(meta, q_ref, own_ref, other_ref, far_ref, far_other_ref, gain_ref, o_ref, s_ref, *, kq):
    cols = lax.broadcasted_iota(jnp.int32, (BLK, BLK), 1)
    rows = lax.broadcasted_iota(jnp.int32, (BLK, BLK), 0)
    limit, me = meta[0], meta[1]
    x, z, c = me // 8, (me // 2) % 4, me % 2
    sg = 1 - 2 * c
    row_base = x * 8 * BLK
    place = [[2 * ((z - flip * r + 4) % 4) + core for r in ROUNDS] for flip, core in ((sg, c), (-sg, 1 - c))]
    diag = place[0][kq]
    heads = TILE // BLK
    blocks = []
    for half, ref in ((0, far_ref), (1, far_other_ref)):
        flip = -sg if half else sg
        for i in range(3):
            source = (x - flip * ROUNDS[i + 1] + 4) % 4
            for k in range(4):
                start = jnp.where(source > x, limit - BLK * (8 * source + place[half][k]), 0)
                blocks.append((ref, (i, k, 0), (i, k, 1), cols >= start))
    for half, ref in ((0, own_ref), (1, other_ref)):
        for k in range(4):
            if half == 0 and k == kq:
                continue
            at = place[half][k]
            cached = (at > diag).astype(jnp.int32) * 2
            start = jnp.where(at > diag, limit - (row_base + at * BLK), 0)
            blocks.append((ref, (k, cached), (k, cached + 1), cols >= start))
    blocks.append((own_ref, (kq, 0), (kq, 1), cols <= rows))
    blocks.append((own_ref, (kq, 2), (kq, 3), (cols > rows) & (cols >= limit - (row_base + diag * BLK))))
    pairs = [blocks[j : j + 2] for j in range(0, len(blocks), 2)]
    for t in range(GROUP // heads):
        q = jnp.concatenate([q_ref[:, (t * heads + h) * BLK : (t * heads + h + 1) * BLK] for h in range(heads)], 0)
        best = None
        for j, pair in enumerate(pairs):
            scores = nt(q, jnp.concatenate([ref[k_at] for ref, k_at, _, _ in pair], 0))
            for u, (_, _, _, mask) in enumerate(pair):
                part = jnp.where(jnp.concatenate([mask] * heads, 0), scores[:, u * BLK : (u + 1) * BLK], MASKED)
                s_ref[t % 2, :, (2 * j + u) * BLK : (2 * j + u + 1) * BLK] = part
                best = part if best is None else jnp.maximum(best, part)
        highest = jnp.max(best, axis=1, keepdims=True) * EXP2_SCALE
        total = None
        for j, pair in enumerate(pairs):
            span = s_ref[t % 2, :, 2 * j * BLK : (2 * j + len(pair)) * BLK]
            weights = jnp.exp2(span * EXP2_SCALE - highest)
            values = jnp.concatenate([ref[v_at] for ref, _, v_at, _ in pair], 0)
            values = jnp.concatenate([values, jnp.ones_like(values)], 1)
            part = jnp.dot(weights.astype(jnp.bfloat16), values, preferred_element_type=jnp.float32)
            total = part if total is None else total + part
        out = (total[:, :BLK] / total[:, BLK:]).astype(jnp.bfloat16)
        for h in range(heads):
            o_ref[:BLK, (t * heads + h) * BLK : (t * heads + h + 1) * BLK] = out[h * BLK : (h + 1) * BLK]
    if kq == 0:
        for g in range(KV_HEADS):
            rows_of = slice(BLK + 16 * g, BLK + 16 * (g + 1))
            part = gain_ref[:, g * GROUP * HEAD : (g + 1) * GROUP * HEAD].astype(jnp.float32)
            o_ref[rows_of, :] = jnp.broadcast_to(part, (16, GROUP * HEAD)).astype(jnp.bfloat16)


def attend(meta, q, own, other, far, far_other, kq, gain):
    vmem = pl.BlockSpec(memory_space=pltpu.VMEM)
    rows = BLK + GAIN_ROWS if kq == 0 else BLK
    return pl.pallas_call(
        functools.partial(attention_kernel, kq=kq),
        out_shape=jax.ShapeDtypeStruct((rows, GROUP * HEAD), jnp.bfloat16),
        in_specs=[pl.BlockSpec(memory_space=pltpu.SMEM)] + [vmem] * 6,
        out_specs=vmem,
        scratch_shapes=[pltpu.VMEM((2, TILE, BLOCKS * BLK), jnp.float32)],
        compiler_params=pltpu.CompilerParams(vmem_limit_bytes=24 * 2**20),
        cost_estimate=pl.CostEstimate(flops=4 * 512 * 4096 * 128, bytes_accessed=2**20, transcendentals=0),
        name="attend",
    )(meta, q, own, other, far, far_other, gain)


def finish_kernel(meta, o0, o1, o2, o3, hidden_ref, out_ref):
    parts = [o[:BLK].astype(jnp.float32) for o in (o0, o1, o2, o3)]
    squares = None
    for part in parts:
        part = part * part
        part = part[:, :128] + part[:, 128:256] + part[:, 256:384] + part[:, 384:]
        squares = part if squares is None else squares + part
    scale = lax.rsqrt(jnp.sum(squares, axis=1, keepdims=True) / (HEADS * HEAD) + 1e-06)
    z, c = (meta[1] // 2) % 4, meta[1] % 2
    for r, part in zip(ROUNDS, parts):
        group = (z + (1 - 2 * c) * r + 4) % 4
        at = pl.ds(pl.multiple_of(group * 512, 512), 512)
        gain = o0[pl.ds(pl.multiple_of(BLK + 16 * group, 16), 16), :].astype(jnp.float32)[:1]
        out_ref[0, :, at] = (hidden_ref[0, :, at].astype(jnp.float32) + part * scale * gain).astype(jnp.bfloat16)


def finish(meta, parts, hidden_before):
    vmem = pl.BlockSpec(memory_space=pltpu.VMEM)
    return pl.pallas_call(
        finish_kernel,
        out_shape=jax.ShapeDtypeStruct((1, BLK, HEADS * HEAD), jnp.bfloat16),
        in_specs=[pl.BlockSpec(memory_space=pltpu.SMEM)] + [vmem] * 5,
        out_specs=vmem,
        compiler_params=pltpu.CompilerParams(vmem_limit_bytes=16 * 2**20),
        name="finish",
    )(meta, *parts, hidden_before)


def on_device(hidden, query_gain, out_gain, keys_now, values_now, keys_cached, values_cached, first_key):
    me = lax.axis_index("seq")
    x, z, c = me // 8, (me // 2) % 4, me % 2
    sg = 1 - 2 * c
    limit = first_key[0]

    def kv_of(head):
        return jnp.stack(
            [
                lax.dynamic_slice(a[0], (0, head * HEAD), (BLK, HEAD))
                for a in (keys_now, values_now, keys_cached, values_cached)
            ]
        )

    hidden_before = lax.ppermute(hidden, "section", [(s, (s + 1) % SECTIONS) for s in range(SECTIONS)])
    pieces = [kv_of(z)]
    for k, r in enumerate(ROUNDS[1:], 1):
        pieces.append(lax.ppermute(kv_of((z + sg * r) % 4), "seq", along_z(r)))
    own = jnp.stack(pieces)

    widened = hidden[0].astype(jnp.float32)
    scale = lax.rsqrt(jnp.mean(widened * widened, axis=-1, keepdims=True) + 1e-06)
    queries = (widened * scale * query_gain[0].astype(jnp.float32)).astype(jnp.bfloat16)

    def q_of(head):
        return lax.dynamic_slice(queries, (0, head * GROUP * HEAD), (BLK, GROUP * HEAD))

    qs = [q_of(z)]
    for k, r in enumerate(ROUNDS[1:], 1):
        qs.append(lax.ppermute(q_of((z + sg * r) % 4), "seq", along_z(r)))

    far = []
    for k, r in enumerate(ROUNDS[1:], 1):
        target = (x + sg * r) % 4
        picked = lax.dynamic_slice_in_dim(own, jnp.where(target > x, 0, 2), 2, 1)
        far.append(lax.ppermute(picked, "seq", along_x(r)))
    other = lax.ppermute(own, "seq", OTHER_CORE)
    far = jnp.stack(far)
    far_other = lax.ppermute(far, "seq", OTHER_CORE)

    meta = jnp.stack([limit, me])
    parts = [None] * 4
    for k in (3, 1, 2, 0):
        attended = attend(meta, qs[k], own, other, far, far_other, k, out_gain)
        parts[k] = lax.ppermute(attended, ("section", "seq"), home_pairs(ROUNDS[k]))
    return finish(meta, parts, hidden_before)


def solution(mesh):
    assert mesh.shape["section"] == SECTIONS and mesh.shape["seq"] == SEQ

    return jax.shard_map(
        on_device,
        mesh=mesh,
        in_specs=(
            P("section", "seq", None),
            P("section", None),
            P("section", None),
            P("section", "seq", None),
            P("section", "seq", None),
            P("section", "seq", None),
            P("section", "seq", None),
            P("section"),
        ),
        out_specs=P("section", "seq", None),
        check_vma=False,
    )
```
